256 devices in a mesh: groups: 2 (over y), lon: 128 (over z, x, core).
Axes of the slice: x: 4, y: 2, z: 16, core: 2. Of those that a mesh axis runs over, the one named last changes fastest.
The devices are a block of a 4x16x16 slice.
Arguments:
- tokens: bfloat16 [8, 24, 768, 512], P('groups', None, 'lon'), parts along dimension 0, may hold values from -6 to 6
- window_shift: int32 [2, 3], replicated, may hold values from 0 to 11, as said below
- fine_gain: float32 [512], replicated, may hold values from 0.25 to 1.75
- fine_qkv: bfloat16 [512, 1536], replicated
- fine_proj: bfloat16 [512, 512], replicated, may hold values from -0.25 to 0.25
- merge_gain: float32 [2048], replicated, may hold values from 0.25 to 1.75
- merge_weight: bfloat16 [2048, 512], replicated, may hold values from -0.125 to 0.125
- coarse_gain: float32 [512], replicated, may hold values from 0.25 to 1.75
- coarse_qkv: bfloat16 [512, 1536], replicated
- coarse_proj: bfloat16 [512, 512], replicated, may hold values from -0.25 to 0.25
- expand_weight: bfloat16 [512, 2048], replicated, may hold values from -0.25 to 0.25
- expand_gain: float32 [512], replicated, may hold values from 0.25 to 1.75
Outputs:
- forecast_state: bfloat16 [8, 24, 768, 512], P('groups', None, 'lon'), parts along dimension 0
The draws below stay inside these ranges and needn't reach their ends.
There are 2 independent parts, one for each index of `groups`. The reference program is written for one: setup_inputs(seed, part) draws one part's arguments, and reference() takes and returns one part's arrays. A program takes and returns all parts, laid end to end along the dimension named above; an argument that names none is the same for every part. Nothing has to cross between parts.
Inputs may be any that keep to these rules, and one draw needn't show every extreme that they name: window_shift[k] holds offsets 0 to 1, 0 to 5 and 0 to 11 along level, latitude and longitude.
All inputs are finite; a program needn't handle non-finite values.
Results may differ from the reference program's by a relative error of at most 0.013.
Values may be sent and summed in bfloat16 or wider, within the bound.
A program may use at most 128 MiB of HBM per device.

```python
import math
import jax
import jax.numpy as jnp
from jax import lax

LEV = 4
LAT = 24
LON_DEV = 6
D = 512
HEADS = 8
DC = 512
HC = 8
WIN_LEV = 2
WIN_LAT = 6
WIN_LON = 12
LON = 768


def projection_draw(key, features):
    base = jax.random.normal(key, (features, 3 * features), jnp.float32) * features ** (-0.5)
    return base.astype(jnp.bfloat16)


def draw_fine_qkv(key, part):
    return projection_draw(jax.random.fold_in(key, 11), D)


def draw_coarse_qkv(key, part):
    return projection_draw(jax.random.fold_in(key, 23), DC)


def draw_window_shift(key, part):
    limits = jnp.array([WIN_LEV, WIN_LAT, WIN_LON], dtype=jnp.int32)
    offsets = jax.random.randint(jax.random.fold_in(key, 37), (2, 3), 0, limits, dtype=jnp.int32)
    chosen = jax.random.randint(jax.random.fold_in(key, 41), (), 0, 2, dtype=jnp.int32)
    row_ids = jnp.arange(2, dtype=jnp.int32)
    lon_col = jnp.where(row_ids == chosen, WIN_LON - 1, offsets[:, 2])
    lev_col = jnp.where(row_ids == chosen, offsets[:, 0], 0)
    offsets = offsets.at[:, 2].set(lon_col)
    offsets = offsets.at[:, 0].set(lev_col)
    return offsets.astype(jnp.int32)


def block_scale(rng, shape, pieces, smallest, top_value):
    def one(dim, shards_of):
        steps = jax.random.uniform(jax.random.fold_in(jax.random.fold_in(rng, 6), dim), (shards_of,), jnp.float32, smallest / len(pieces), top_value / len(pieces))
        return jnp.repeat(jnp.exp(steps), shape[dim] // shards_of).reshape((-1,) + (1,) * (len(shape) - dim - 1))

    level = one(*pieces[0])
    for cut in pieces[1:]:
        level = level * one(*cut)
    return level


def gaussian(rng, shape, scale, bound, shards=(), kind=jnp.bfloat16):
    level = block_scale(rng, shape, shards, -0.22, 0.18) if shards else 1.0
    entries = jax.random.normal(rng, shape, jnp.float32) * scale * level
    return jnp.minimum(jnp.maximum(entries, -bound), bound).astype(kind)


def setup_inputs(seed: int = 0, part: int = 0) -> dict:
    key_list = jax.random.split(jax.random.key(seed), 13)
    part_keys = jax.random.split(jax.random.fold_in(key_list[12], part), 13)
    tokens = gaussian(part_keys[0], (LEV, LAT, LON, D), 1.0, 6.0, ((2, 128),))
    window_shift = draw_window_shift(jax.random.fold_in(key_list[12], 71), part)
    fine_gain = jnp.clip(1.0 + 0.15 * jax.random.normal(key_list[2], (D,), jnp.float32), 0.25, 1.75)
    fine_qkv = draw_fine_qkv(jax.random.fold_in(key_list[12], 71), part)
    fine_proj = gaussian(key_list[4], (D, D), D ** -0.5, 0.25)
    merge_gain = jnp.clip(1.0 + 0.15 * jax.random.normal(key_list[5], (4 * D,), jnp.float32), 0.25, 1.75)
    merge_weight = gaussian(key_list[6], (4 * D, DC), (4 * D) ** -0.5, 0.125)
    coarse_gain = jnp.clip(1.0 + 0.15 * jax.random.normal(key_list[7], (DC,), jnp.float32), 0.25, 1.75)
    coarse_qkv = draw_coarse_qkv(jax.random.fold_in(key_list[12], 71), part)
    coarse_proj = gaussian(key_list[9], (DC, DC), DC ** -0.5, 0.25)
    expand_weight = gaussian(key_list[10], (DC, 4 * D), DC ** -0.5, 0.25)
    expand_gain = jnp.clip(1.0 + 0.15 * jax.random.normal(key_list[11], (D,), jnp.float32), 0.25, 1.75)
    return dict(tokens=tokens, window_shift=window_shift, fine_gain=fine_gain, fine_qkv=fine_qkv, fine_proj=fine_proj, merge_gain=merge_gain, merge_weight=merge_weight, coarse_gain=coarse_gain, coarse_qkv=coarse_qkv, coarse_proj=coarse_proj, expand_weight=expand_weight, expand_gain=expand_gain)


EPSILON = 1e-05

def layer_norm(inputs, gain_vec):
    inputs = inputs.astype(jnp.float32)
    center = inputs - lax.optimization_barrier(jnp.mean(inputs, axis=-1, keepdims=True))
    spread = lax.optimization_barrier(jnp.mean(center * center, axis=-1, keepdims=True))
    return center * lax.rsqrt(spread + EPSILON) * gain_vec

def rolled_ids(length, offset, extent):
    placed = jnp.arange(length, dtype=jnp.int32)
    source = (placed - offset) % length
    return (source + offset) // extent

def roll_grid(tensor_in, offsets, factor):
    return jnp.roll(jnp.roll(tensor_in, factor * offsets[0], 0), factor * offsets[1], 1)

def window_attention(queries, key_block, value_block, query_cols, key_cols, offsets, lon_total, head_count):
    levels, lat_rows, query_wide, features = queries.shape
    key_wide = key_block.shape[2]
    head_size = features // head_count
    lev_blocks = levels // WIN_LEV
    lat_blocks = lat_rows // WIN_LAT

    def blocked(tensor_in, wide_cols):
        tensor_in = tensor_in.reshape(lev_blocks, WIN_LEV, lat_blocks, WIN_LAT, wide_cols, head_count, head_size)
        tensor_in = tensor_in.transpose(0, 2, 1, 3, 4, 5, 6)
        return tensor_in.reshape(lev_blocks * lat_blocks, WIN_LEV * WIN_LAT * wide_cols, head_count, head_size)
    lev_ids = rolled_ids(levels, offsets[0], WIN_LEV).reshape(lev_blocks, WIN_LEV)
    row_ids = rolled_ids(lat_rows, offsets[1], WIN_LAT).reshape(lat_blocks, WIN_LAT)
    lev_same = lev_ids[:, :, None] == lev_ids[:, None, :]
    row_same = row_ids[:, :, None] == row_ids[:, None, :]
    query_win = (query_cols + offsets[2]) % lon_total // WIN_LON
    key_win = (key_cols + offsets[2]) % lon_total // WIN_LON
    col_same = query_win[:, None] == key_win[None, :]
    allowed = lev_same[:, None, :, None, None, :, None, None] & row_same[None, :, None, :, None, None, :, None] & col_same[None, None, None, None, :, None, None, :]
    allowed = allowed.reshape(lev_blocks * lat_blocks, WIN_LEV * WIN_LAT * query_wide, WIN_LEV * WIN_LAT * key_wide)
    query_b = blocked(queries, query_wide).astype(jnp.float32)
    key_b = blocked(key_block, key_wide).astype(jnp.float32)
    value_b = blocked(value_block, key_wide).astype(jnp.float32)
    scores = jnp.einsum('bqhd,bkhd->bhqk', query_b, key_b) / math.sqrt(head_size)
    scores = jnp.where(allowed[:, None], scores, -1e+30)
    row_max = lax.optimization_barrier(jnp.max(scores, axis=-1, keepdims=True))
    expo = jnp.exp(scores - row_max)
    weight = (expo / lax.optimization_barrier(jnp.sum(expo, axis=-1, keepdims=True))).astype(jnp.bfloat16)
    mixture = jnp.einsum('bhqk,bkhd->bqhd', weight.astype(jnp.float32), value_b).astype(jnp.bfloat16)
    mixture = mixture.reshape(lev_blocks, lat_blocks, WIN_LEV, WIN_LAT, query_wide, features)
    return mixture.transpose(0, 2, 1, 3, 4, 5).reshape(levels, lat_rows, query_wide, features)

def attention_block(grid, gain_vec, qkv_weight, proj_weight, offsets, head_count, block_cols):
    levels, lat_rows, lon_total, features = grid.shape
    reach = WIN_LON - 1
    normed = layer_norm(grid, gain_vec).astype(jnp.bfloat16)
    projected = jnp.dot(normed, qkv_weight, preferred_element_type=jnp.float32).astype(jnp.bfloat16)
    queries = roll_grid(projected[..., :features], offsets, 1)
    key_block = roll_grid(projected[..., features:2 * features], offsets, 1)
    value_block = roll_grid(projected[..., 2 * features:], offsets, 1)

    def one_block(index):
        first_col = index * block_cols
        query_cols = first_col + jnp.arange(block_cols, dtype=jnp.int32)
        key_cols = (first_col - reach + jnp.arange(block_cols + 2 * reach, dtype=jnp.int32)) % lon_total
        query_part = lax.dynamic_slice_in_dim(queries, first_col, block_cols, 2)
        key_part = jnp.take(key_block, key_cols, axis=2)
        value_part = jnp.take(value_block, key_cols, axis=2)
        return window_attention(query_part, key_part, value_part, query_cols, key_cols, offsets, lon_total, head_count)
    outputs = lax.map(one_block, jnp.arange(lon_total // block_cols, dtype=jnp.int32))
    outputs = outputs.transpose(1, 2, 0, 3, 4).reshape(levels, lat_rows, lon_total, features)
    outputs = roll_grid(outputs, offsets, -1)
    update = jnp.dot(outputs, proj_weight, preferred_element_type=jnp.float32)
    return (grid.astype(jnp.float32) + update).astype(jnp.bfloat16)

def merge_patches(fine, gain_vec, weight):
    levels, lat_rows, lon_cols, features = fine.shape
    grouped = fine.reshape(levels, lat_rows // 2, 2, lon_cols // 2, 2, features)
    grouped = grouped.transpose(0, 1, 3, 4, 2, 5).reshape(levels, lat_rows // 2, lon_cols // 2, 4 * features)
    merged = layer_norm(grouped, gain_vec).astype(jnp.bfloat16)
    return jnp.dot(merged, weight, preferred_element_type=jnp.float32).astype(jnp.bfloat16)

def expand_patches(coarse, weight, gain_vec, fine):
    levels, lat_rows, lon_cols, channels = coarse.shape
    features = fine.shape[-1]
    expanded = jnp.dot(coarse, weight, preferred_element_type=jnp.float32)
    expanded = layer_norm(expanded.reshape(levels, lat_rows, lon_cols, 2, 2, features), gain_vec)
    expanded = expanded.transpose(0, 1, 4, 2, 3, 5).reshape(levels, 2 * lat_rows, 2 * lon_cols, features)
    return (fine.astype(jnp.float32) + expanded).astype(jnp.bfloat16)

def reference(tokens, window_shift, fine_gain, fine_qkv, fine_proj, merge_gain, merge_weight, coarse_gain, coarse_qkv, coarse_proj, expand_weight, expand_gain):
    fine = attention_block(tokens, fine_gain, fine_qkv, fine_proj, window_shift[0], HEADS, LON_DEV)
    coarse = merge_patches(fine, merge_gain, merge_weight)
    coarse = attention_block(coarse, coarse_gain, coarse_qkv, coarse_proj, window_shift[1], HC, LON_DEV // 2)
    return expand_patches(coarse, expand_weight, expand_gain, fine)
```

```python
import functools
import math

import jax
import jax.numpy as jnp
from jax import lax
from jax.experimental import pallas as pl
from jax.experimental.pallas import tpu as pltpu
from jax.sharding import PartitionSpec as P

HEADS = 8
WIN_LEV = 2
WIN_LAT = 6
WIN_LON = 12
EPSILON = 1e-05
MASKED = -1e30
MESH = pl.DeviceIdType.MESH
VMEM_LIMIT = 62 * 1024 * 1024


def div(value, by):
    return (value * ((2**20 + by - 1) // by)) >> 20


def iota(shape, dim):
    return lax.broadcasted_iota(jnp.int32, shape, dim)


def one_hot(source, width):
    rows = source.shape[0]
    return (source == iota((rows, width), 1)).astype(jnp.float32).astype(jnp.bfloat16)


def norm(values, gain):
    mean = jnp.mean(values, axis=-1, keepdims=True)
    center = values - mean
    spread = jnp.mean(center * center, axis=-1, keepdims=True)
    return center * lax.rsqrt(spread + EPSILON) * gain


def matmul(left, right):
    return jnp.dot(left, right, preferred_element_type=jnp.float32)


def matmul_nt(left, right):
    return lax.dot_general(
        left, right, (((1,), (1,)), ((), ())), preferred_element_type=jnp.float32
    )


def attend(q_ref, k_ref, v_ref, bias_ref, out_ref):
    rows = q_ref.shape[0]
    width = 128
    head = width // 2
    first = iota((rows, width), 1) < head

    def pair(index, carry):
        lanes = pl.ds(pl.multiple_of(index * width, width), width)
        q = q_ref[:, lanes]
        zero = jnp.zeros_like(q)
        stacked = jnp.concatenate([jnp.where(first, q, zero), jnp.where(first, zero, q)], axis=0)
        scores = matmul_nt(stacked, k_ref[:, lanes])
        bias = bias_ref[...]
        scores = scores + jnp.concatenate([bias, bias], axis=0)
        top = jnp.max(scores, axis=-1, keepdims=True)
        expo = jnp.exp(scores - top)
        total = jnp.sum(expo, axis=-1, keepdims=True)
        mix = matmul(expo.astype(jnp.bfloat16), v_ref[:, lanes]) / total
        out_ref[:, lanes] = jnp.where(first, mix[:rows], mix[rows:]).astype(jnp.bfloat16)
        return carry

    lax.fori_loop(0, q_ref.shape[1] // width, pair, 0)


def roll_kernel(shift_ref, tokens_ref, out_ref, padded):
    levels, lat_rows, cols, features = tokens_ref.shape
    lat_shift = shift_ref[0, 1]
    padded[...] = jnp.zeros_like(padded)
    for level in range(levels):
        padded[level, :, 0:cols, :] = tokens_ref[level].astype(jnp.float32)
    flat = padded[...].reshape(levels * lat_rows * 8, features).astype(jnp.bfloat16)
    group = cols * levels * WIN_LAT
    for window in range(lat_rows // WIN_LAT):
        row = iota((group, 1), 0)
        col = div(row, levels * WIN_LAT)
        rest = row - col * (levels * WIN_LAT)
        level = div(rest, WIN_LAT)
        lat = window * WIN_LAT + rest - level * WIN_LAT - lat_shift
        lat = jnp.where(lat < 0, lat + lat_rows, lat)
        source = (level * lat_rows + lat) * 8 + col
        out_ref[window] = matmul(one_hot(source, flat.shape[0]), flat).astype(jnp.bfloat16)


def main_kernel(
    devices,
    shift_ref,
    x_ref,
    fine_gain_ref,
    merge_gain_ref,
    coarse_gain_ref,
    fine_qkv_hbm,
    fine_proj_hbm,
    merge_hbm,
    coarse_qkv_hbm,
    coarse_proj_hbm,
    fine_out_ref,
    coarse_out_ref,
    fine_qkv,
    fine_proj,
    merge_weight,
    coarse_qkv,
    coarse_proj,
    halo,
    normed,
    q_buf,
    k_buf,
    v_buf,
    bias,
    mix,
    fine_rolled,
    coarse_buf,
    coarse_halo,
    ckey,
    cvalue,
    cbias,
    weight_sem,
    send_sem,
    recv_sem,
    csend_sem,
    crecv_sem,
):
    windows, group, features = x_ref.shape
    levels = 4
    lat_rows = windows * WIN_LAT
    per_col = levels * WIN_LAT
    cols = group // per_col
    part = 128
    me = lax.axis_index("lon")
    parity = lax.rem(me, 2)
    side = 2 * parity - 1
    cgroup = coarse_buf.shape[0]
    ccols = cols // 2
    clat = lat_rows // 2
    cper = levels * clat
    cpart = 2 * cper

    def device(steps):
        return {"lon": lax.rem(me + steps * side + 4 * devices, devices)}

    def weight_copy(index, source, target):
        return pltpu.make_async_copy(source, target, weight_sem.at[index])

    weights = [
        weight_copy(0, fine_qkv_hbm, fine_qkv),
        weight_copy(1, fine_proj_hbm, fine_proj),
        weight_copy(2, merge_hbm, merge_weight),
        weight_copy(3, coarse_qkv_hbm, coarse_qkv),
        weight_copy(4, coarse_proj_hbm, coarse_proj),
    ]
    for copy in weights:
        copy.start()

    barrier = pltpu.get_barrier_semaphore()
    for steps in (1, -1, 2, -2, 3, 4, -4):
        pl.semaphore_signal(barrier, inc=1, device_id=device(steps), device_id_type=MESH)
    pl.semaphore_wait(barrier, 7)

    near = pl.multiple_of(16 * (1 - parity), 16)

    def remote(source, target, kind, index, steps, sends, recvs):
        return pltpu.make_async_remote_copy(
            src_ref=source,
            dst_ref=target,
            send_sem=sends.at[kind, index],
            recv_sem=recvs.at[kind, index],
            device_id=device(steps),
            device_id_type=MESH,
        )

    def fine_copy(kind, w):
        if kind == 0:
            return remote(x_ref.at[w], halo.at[w, pl.ds(0, group)], 0, w, 1, send_sem, recv_sem)
        if kind == 1:
            target = halo.at[w, pl.ds(group, group)]
            return remote(x_ref.at[w], target, 1, w, -1, send_sem, recv_sem)
        if kind == 2:
            target = halo.at[w, pl.ds(2 * group, part)]
            return remote(
                x_ref.at[w, pl.ds(near, part)], target, 2, w, -2, send_sem, recv_sem
            )
        target = halo.at[w, pl.ds(2 * group + part, part)]
        return remote(halo.at[w, pl.ds(near, part)], target, 3, w, -1, send_sem, recv_sem)

    for w in range(windows):
        for kind in range(3):
            fine_copy(kind, w).start()

    lev_shift = shift_ref[0, 0]
    lat_shift = shift_ref[0, 1]
    lon_shift = shift_ref[0, 2] + lax.rem(me * cols, WIN_LON) + 2 * WIN_LON

    def fine_ids(row, steps, w):
        col = div(row, per_col)
        rest = row - col * per_col
        level = div(rest, WIN_LAT)
        lat = rest - level * WIN_LAT
        win = div(col + cols * steps + lon_shift, WIN_LON)
        wrapped = jnp.where(w * lat_rows + lat < lat_shift, 1, 0)
        return (win * 4 + ((level + lev_shift) >> 1)) * 2 + wrapped

    keys = 3 * group + 2 * part
    spot = iota((1, keys), 1)
    slot = div(spot, group)
    row = spot - slot * group
    steps = jnp.where(slot == 0, 0, jnp.where(slot == 1, side, -side))
    far_out = (spot >= 3 * group) & (spot < 3 * group + part)
    far_in = spot >= 3 * group + part
    steps = jnp.where(far_out, 2 * side, jnp.where(far_in, -2 * side, steps))
    row = jnp.where(far_out, spot - 3 * group, jnp.where(far_in, spot - 3 * group - part, row))
    row = jnp.where((spot >= 3 * group) & (steps < 0), row + 16, row)
    gain = fine_gain_ref[...]

    weights[0].wait()

    def fine_kv(start, size):
        piece = normed[pl.ds(start, size), :]
        kv = matmul(piece, fine_qkv[:, features:])
        k_buf[pl.ds(start, size), :] = kv[:, :features].astype(jnp.bfloat16)
        v_buf[pl.ds(start, size), :] = kv[:, features:].astype(jnp.bfloat16)

    def fine_window(w, carry):
        own = x_ref[w]
        query_id = fine_ids(iota((group, 1), 0), 0, w)
        key_id = fine_ids(row, steps, w)
        bias[...] = jnp.where(query_id == key_id, 0.0, MASKED)
        normed[0:group, :] = norm(own.astype(jnp.float32), gain).astype(jnp.bfloat16)
        q = matmul(normed[0:group, :], fine_qkv[:, :features]).astype(jnp.bfloat16)
        q_buf[...] = q * jnp.bfloat16(1.0 / math.sqrt(features // HEADS))
        fine_copy(0, w).wait_recv()
        fine_copy(3, w).start()
        fine_copy(1, w).wait_recv()
        normed[group : 3 * group, :] = norm(
            halo[w, 0 : 2 * group, :].astype(jnp.float32), gain
        ).astype(jnp.bfloat16)
        fine_kv(0, 3 * group)
        fine_copy(2, w).wait_recv()
        fine_copy(3, w).wait_recv()
        normed[3 * group :, :] = norm(
            halo[w, 2 * group :, :].astype(jnp.float32), gain
        ).astype(jnp.bfloat16)
        fine_kv(3 * group, 2 * part)
        attend(q_buf, k_buf, v_buf, bias, mix)
        update = matmul(mix[...], fine_proj[...])
        fine_rolled[pl.ds(pl.multiple_of(w * group, 16), group), :] = (
            own.astype(jnp.float32) + update
        ).astype(jnp.bfloat16)
        return carry

    weights[1].wait()
    lax.fori_loop(0, windows, fine_window, 0)

    crow = iota((cgroup, 1), 0)
    ccol = div(crow, cper)
    rest = crow - ccol * cper
    clevel = div(rest, clat)
    clat_row = rest - clevel * clat
    fine_all = fine_rolled[...]
    total = jnp.zeros((cgroup, 1), jnp.float32)
    pieces = []
    for piece in range(4):
        lat = 2 * clat_row + piece % 2 + lat_shift
        lat = jnp.where(lat >= lat_rows, lat - lat_rows, lat)
        window = div(lat, WIN_LAT)
        source = (
            window * group
            + (2 * ccol + piece // 2) * per_col
            + clevel * WIN_LAT
            + lat
            - window * WIN_LAT
        )
        picked = matmul(one_hot(source, windows * group), fine_all)
        fine_out_ref[piece] = picked.astype(jnp.bfloat16)
        pieces.append(picked)
        total = total + jnp.sum(picked, axis=-1, keepdims=True)
    mean = total / (4 * features)
    square = jnp.zeros((cgroup, 1), jnp.float32)
    for piece in range(4):
        pieces[piece] = pieces[piece] - mean
        square = square + jnp.sum(pieces[piece] * pieces[piece], axis=-1, keepdims=True)
    scale = lax.rsqrt(square / (4 * features) + EPSILON)
    weights[2].wait()
    coarse = jnp.zeros((cgroup, features), jnp.float32)
    for piece in range(4):
        merged = pieces[piece] * scale * merge_gain_ref[pl.ds(piece, 1), :]
        coarse = coarse + matmul(
            merged.astype(jnp.bfloat16), merge_weight[pl.ds(piece * features, features), :]
        )
    coarse_buf[...] = coarse.astype(jnp.bfloat16)

    clev_shift = shift_ref[1, 0]
    clat_shift = shift_ref[1, 1]
    clon_shift = shift_ref[1, 2] + lax.rem(me * ccols, WIN_LON) + 2 * WIN_LON

    def coarse_ids(row, steps):
        col = div(row, cper)
        rest = row - col * cper
        level = div(rest, clat)
        lat = rest - level * clat
        win = div(col + ccols * steps + clon_shift, WIN_LON)
        return (win * 4 + ((level + clev_shift) >> 1)) * 4 + div(lat + clat_shift, WIN_LAT)

    ckeys = 7 * cgroup + 2 * cpart
    spot = iota((1, ckeys), 1)
    slot = div(spot, cgroup)
    crow = spot - slot * cgroup
    csteps = jnp.zeros_like(spot)
    for number, amount in enumerate((0, 1, -1, 2, 3, -2, -3)):
        csteps = jnp.where(slot == number, amount * side, csteps)
    far_out = (spot >= 7 * cgroup) & (spot < 7 * cgroup + cpart)
    far_in = spot >= 7 * cgroup + cpart
    csteps = jnp.where(far_out, 4 * side, jnp.where(far_in, -4 * side, csteps))
    crow = jnp.where(
        far_out, spot - 7 * cgroup, jnp.where(far_in, spot - 7 * cgroup - cpart, crow)
    )
    crow = jnp.where((spot >= 7 * cgroup) & (csteps < 0), crow + cper, crow)
    query_id = coarse_ids(iota((cgroup, 1), 0), 0)
    cbias[...] = jnp.where(query_id == coarse_ids(crow, csteps), 0.0, MASKED)

    cnear = pl.multiple_of(cper * (1 - parity), 16)
    starts = {1: 0, -1: cgroup, 2: 2 * cgroup, 3: 3 * cgroup, -2: 4 * cgroup, -3: 5 * cgroup}
    starts[4] = 6 * cgroup
    starts[-4] = 6 * cgroup + cpart

    def coarse_remote(kind, source, slot, size, steps):
        return remote(
            source, coarse_halo.at[pl.ds(starts[slot], size)], kind, 0, steps, csend_sem, crecv_sem
        )

    whole = coarse_buf
    ccopies = {
        1: coarse_remote(0, whole, 1, cgroup, 1),
        -1: coarse_remote(1, whole, -1, cgroup, -1),
        2: coarse_remote(2, whole, 2, cgroup, -2),
        3: coarse_remote(3, whole, 3, cgroup, 3),
        4: coarse_remote(4, whole.at[pl.ds(cnear, cpart)], 4, cpart, -4),
        -2: coarse_remote(5, coarse_halo.at[pl.ds(starts[1], cgroup)], -2, cgroup, -1),
        -3: coarse_remote(6, coarse_halo.at[pl.ds(starts[2], cgroup)], -3, cgroup, -1),
        -4: coarse_remote(
            7, coarse_halo.at[pl.ds(pl.multiple_of(starts[3] + cnear, 16), cpart)], -4, cpart, -1
        ),
    }
    for slot in (1, 2, 3, 4, -1):
        ccopies[slot].start()

    cgain = coarse_gain_ref[...]
    weights[3].wait()

    def coarse_kv(values, start, size):
        piece = norm(values.astype(jnp.float32), cgain).astype(jnp.bfloat16)
        kv = matmul(piece, coarse_qkv[:, features:])
        ckey[pl.ds(start, size), :] = kv[:, :features].astype(jnp.bfloat16)
        cvalue[pl.ds(start, size), :] = kv[:, features:].astype(jnp.bfloat16)
        return piece

    piece = coarse_kv(coarse_buf[...], 0, cgroup)
    q = matmul(piece, coarse_qkv[:, :features]).astype(jnp.bfloat16)
    q_buf[...] = q * jnp.bfloat16(1.0 / math.sqrt(features // HEADS))
    for slot, relay in ((-1, None), (1, -2), (2, -3), (3, -4), (-2, None), (-3, None), (4, None), (-4, None)):
        ccopies[slot].wait_recv()
        if relay is not None:
            ccopies[relay].start()
        size = cpart if abs(slot) == 4 else cgroup
        coarse_kv(coarse_halo[pl.ds(starts[slot], size), :], cgroup + starts[slot], size)
    attend(q_buf, ckey, cvalue, cbias, mix)
    weights[4].wait()
    update = matmul(mix[...], coarse_proj[...])
    coarse_out_ref[...] = (coarse_buf[...].astype(jnp.float32) + update).astype(jnp.bfloat16)

    for slot in (1, -1, 2, 3, 4, -2, -3, -4):
        ccopies[slot].wait_send()
    for w in range(windows):
        for kind in range(4):
            fine_copy(kind, w).wait_send()


def expand_kernel(fine_ref, coarse_ref, weight_ref, gain_ref, out_ref, joined):
    levels, lat_rows, cols, features = out_ref.shape
    group = coarse_ref.shape[0]
    clat = lat_rows // 2
    cper = levels * clat
    gain = gain_ref[...]
    coarse = coarse_ref[...]
    for piece in range(4):
        expanded = matmul(coarse, weight_ref[:, piece * features : (piece + 1) * features])
        joined[piece * group : (piece + 1) * group, :] = (
            fine_ref[piece].astype(jnp.float32) + norm(expanded, gain)
        ).astype(jnp.bfloat16)
    pieces = joined[...]
    row = iota((lat_rows * 8, 1), 0)
    lat = row >> 3
    col = row & 7
    for level in range(levels):
        source = (
            (2 * (col & 1) + (lat & 1)) * group + (col >> 1) * cper + level * clat + (lat >> 1)
        )
        source = jnp.where(col < cols, source, -1)
        picked = matmul(one_hot(source, 4 * group), pieces)
        picked = picked.reshape(lat_rows, 8, features)[:, :cols, :]
        out_ref[level] = picked.astype(jnp.bfloat16)


def local(
    tokens,
    window_shift,
    fine_gain,
    fine_qkv,
    fine_proj,
    merge_gain,
    merge_weight,
    coarse_gain,
    coarse_qkv,
    coarse_proj,
    expand_weight,
    expand_gain,
):
    devices = lax.axis_size("lon")
    levels, lat_rows, cols, features = tokens.shape
    windows = lat_rows // WIN_LAT
    group = cols * levels * WIN_LAT
    cgroup = levels * (lat_rows // 2) * (cols // 2)
    cpart = 2 * levels * (lat_rows // 2)
    part = 128
    keys = 3 * group + 2 * part
    ckeys = 7 * cgroup + 2 * cpart
    bf16 = jnp.bfloat16
    vmem = pl.BlockSpec(memory_space=pltpu.VMEM)
    smem = pl.BlockSpec(memory_space=pltpu.SMEM)
    anywhere = pl.BlockSpec(memory_space=pl.ANY)
    rolled = pl.pallas_call(
        roll_kernel,
        out_shape=jax.ShapeDtypeStruct((windows, group, features), bf16),
        in_specs=[smem, vmem],
        out_specs=vmem,
        scratch_shapes=[pltpu.VMEM((levels, lat_rows, 8, features), jnp.float32)],
        compiler_params=pltpu.CompilerParams(vmem_limit_bytes=VMEM_LIMIT),
        name="roll",
    )(window_shift, tokens)
    fine, coarse = pl.pallas_call(
        functools.partial(main_kernel, devices),
        out_shape=(
            jax.ShapeDtypeStruct((4, cgroup, features), bf16),
            jax.ShapeDtypeStruct((cgroup, features), bf16),
        ),
        in_specs=[smem] + [vmem] * 4 + [anywhere] * 5,
        out_specs=(vmem, vmem),
        scratch_shapes=[
            pltpu.VMEM(fine_qkv.shape, bf16),
            pltpu.VMEM(fine_proj.shape, bf16),
            pltpu.VMEM(merge_weight.shape, bf16),
            pltpu.VMEM(coarse_qkv.shape, bf16),
            pltpu.VMEM(coarse_proj.shape, bf16),
            pltpu.VMEM((windows, keys - group, features), bf16),
            pltpu.VMEM((keys, features), bf16),
            pltpu.VMEM((group, features), bf16),
            pltpu.VMEM((keys, features), bf16),
            pltpu.VMEM((keys, features), bf16),
            pltpu.VMEM((group, keys), jnp.float32),
            pltpu.VMEM((group, features), bf16),
            pltpu.VMEM((windows * group, features), bf16),
            pltpu.VMEM((cgroup, features), bf16),
            pltpu.VMEM((ckeys - cgroup, features), bf16),
            pltpu.VMEM((ckeys, features), bf16),
            pltpu.VMEM((ckeys, features), bf16),
            pltpu.VMEM((cgroup, ckeys), jnp.float32),
            pltpu.SemaphoreType.DMA((5,)),
            pltpu.SemaphoreType.DMA((4, windows)),
            pltpu.SemaphoreType.DMA((4, windows)),
            pltpu.SemaphoreType.DMA((8, 1)),
            pltpu.SemaphoreType.DMA((8, 1)),
        ],
        compiler_params=pltpu.CompilerParams(
            collective_id=0, has_side_effects=True, vmem_limit_bytes=VMEM_LIMIT
        ),
        name="encode",
    )(
        window_shift,
        rolled,
        fine_gain.reshape(1, features),
        merge_gain.reshape(4, features),
        coarse_gain.reshape(1, features),
        fine_qkv,
        fine_proj,
        merge_weight,
        coarse_qkv,
        coarse_proj,
    )
    return pl.pallas_call(
        expand_kernel,
        out_shape=jax.ShapeDtypeStruct(tokens.shape, tokens.dtype),
        in_specs=[vmem] * 4,
        out_specs=vmem,
        scratch_shapes=[pltpu.VMEM((4 * cgroup, features), bf16)],
        compiler_params=pltpu.CompilerParams(vmem_limit_bytes=VMEM_LIMIT),
        name="expand",
    )(fine, coarse, expand_weight, expand_gain.reshape(1, features))


def solution(mesh):
    placed = (P("groups", None, "lon", None), P(), P(), P(), P(), P(), P(), P(), P(), P(), P(), P())
    return jax.shard_map(
        local, mesh=mesh, in_specs=placed, out_specs=P("groups", None, "lon", None), check_vma=False
    )
```
